512 devices in a mesh: groups: 2 (over y), rows: 128 (over z, x), sub: 2 (over core).
Axes of the slice: x: 4, y: 2, z: 32, core: 2. Of those that a mesh axis runs over, the one named last changes fastest.
The devices are a block of a 4x8x32 slice.
Arguments:
- residuals: bfloat16 [32768, 2048], P(('groups', 'rows'), 'sub'), parts along dimension 0, may hold values from -96 to 96
- codes: int32 [32768, 256], P(('groups', 'rows'), 'sub'), parts along dimension 0, may hold values from 0 to 127
- codebook: float32 [512, 8, 128], P(('groups', 'sub')), parts along dimension 0, may hold values from -4 to 4
Outputs:
- refined: float32 [512, 8, 128], P(('groups', 'sub')), parts along dimension 0
The draws below stay inside these ranges and needn't reach their ends.
There are 2 independent parts, one for each index of `groups`. The reference program is written for one: setup_inputs(seed, part) draws one part's arguments, and reference() takes and returns one part's arrays. A program takes and returns all parts, laid end to end along the dimension named above; each array names one. Nothing has to cross between parts.
All inputs are finite; a program needn't handle non-finite values.
Results may differ from the reference program's by a relative error of at most 0.0037.
Values sent between devices are 32-bit elements; how exact they have to be, the bound alone decides.
No kernel may reach another device: no remote copies, remote signals or barrier semaphores. Data moves between devices by JAX's collectives and lax.ppermute only.
A program may use at most 64 MiB of HBM per device.

```python
import jax
import jax.numpy as jnp
from jax import lax

SUBSPACES = 256
SUBDIM = 8
CODEWORDS = 128
VECTORS = 16384


def true_codes(key):
    return jax.random.randint(jax.random.fold_in(jax.random.fold_in(key, 11), 2), (VECTORS, SUBSPACES), 0, CODEWORDS, dtype=jnp.int32)


def draw_codes(key, part):
    truth = true_codes(key)
    base = jax.random.fold_in(key, 12)
    swapped = jax.random.randint(jax.random.fold_in(base, 1), (VECTORS, SUBSPACES), 0, 10, dtype=jnp.int32) < 3
    other = jax.random.randint(jax.random.fold_in(base, 2), (VECTORS, SUBSPACES), 0, CODEWORDS, dtype=jnp.int32)
    return jnp.where(swapped, other, truth)


def draw_residuals(key, part):
    truth = true_codes(key)
    centers = jax.random.truncated_normal(jax.random.fold_in(jax.random.fold_in(key, 11), 1), -3.0, 3.0, (SUBSPACES, CODEWORDS, SUBDIM), jnp.float32)
    picked = centers[jnp.arange(SUBSPACES, dtype=jnp.int32)[None, :], truth]
    noise = jax.random.truncated_normal(jax.random.fold_in(key, 21), -3.0, 3.0, (VECTORS, SUBSPACES, SUBDIM), jnp.float32)
    vectors = picked + noise
    return vectors.reshape(VECTORS, SUBSPACES * SUBDIM).astype(jnp.bfloat16)


def block_scale(own_key, shape, split, least, largest):
    factor_of = 1.0
    for position, shards_of in split:
        steps = jax.random.uniform(jax.random.fold_in(jax.random.fold_in(own_key, 6), position), (shards_of,), jnp.float32, least / len(split), largest / len(split))
        factor_of = factor_of * jnp.repeat(jnp.exp(steps), shape[position] // shards_of).reshape((-1,) + (1,) * (len(shape) - 1 - position))
    return factor_of


def gaussian(stream_key, shape, width, bound, pieces=(), held_as=jnp.bfloat16):
    result = jax.random.normal(stream_key, shape, jnp.float32) * width
    if len(pieces) > 0:
        result = block_scale(stream_key, shape, pieces, -0.22, 0.18) * result
    return jnp.clip(result, min=-bound, max=bound).astype(held_as)


def setup_inputs(seed: int = 0, part: int = 0) -> dict:
    seeds = jax.random.split(jax.random.key(seed), 4)
    part_keys = jax.random.split(jax.random.fold_in(seeds[3], part), 4)
    return {
        "residuals": draw_residuals(jax.random.fold_in(jax.random.fold_in(seeds[3], part), 71), part),
        "codes": draw_codes(jax.random.fold_in(jax.random.fold_in(seeds[3], part), 71), part),
        "codebook": gaussian(part_keys[2], (SUBSPACES, SUBDIM, CODEWORDS), 1.0, 4.0, ((0, 2),), jnp.float32),
    }


def renew(prior, sums, counts, lam):
    return (sums + lam * prior) / (counts[:, None, :] + lam)


def reference(residuals, codes, codebook):
    lam = VECTORS / (8.0 * CODEWORDS)
    levels = jnp.arange(CODEWORDS, dtype=jnp.int32)
    index = jnp.arange(SUBSPACES, dtype=jnp.int32)

    def first(m):
        cols = lax.dynamic_slice_in_dim(residuals, m * SUBDIM, SUBDIM, 1).astype(jnp.float32)
        column = lax.dynamic_slice_in_dim(codes, m, 1, 1)
        onehot = (column == levels[None, :]).astype(jnp.float32)
        sums = jnp.dot(cols.T, onehot, precision=lax.Precision.HIGHEST, preferred_element_type=jnp.float32)
        return sums, jnp.sum(onehot, axis=0)

    sums1, counts1 = lax.map(first, index)
    book1 = renew(codebook, sums1, counts1, lam)

    def second(m):
        cols = lax.dynamic_slice_in_dim(residuals, m * SUBDIM, SUBDIM, 1)
        center = book1[m]
        cross = jnp.dot(cols, center.astype(jnp.bfloat16), preferred_element_type=jnp.float32)
        scores = 2.0 * cross - jnp.sum(center * center, axis=0)[None, :]
        weights = jax.nn.softmax(scores, axis=1).astype(jnp.bfloat16)
        sums = jnp.dot(cols.T, weights, preferred_element_type=jnp.float32)
        return sums, jnp.sum(weights.astype(jnp.float32), axis=0)

    sums2, counts2 = lax.map(second, index)
    return renew(book1, sums2, counts2, lam)
```

```python
import functools

import jax
import jax.numpy as jnp
from jax import lax
from jax.experimental import pallas as pl
from jax.experimental.pallas import tpu as pltpu
from jax.sharding import Mesh
from jax.sharding import PartitionSpec as P

ROWS = ("rows_0", "rows_1", "rows_2")
GROUPS_ROWS = ("groups", *ROWS)
NT = (((1,), (1,)), ((), ()))
f32, bf16 = jnp.float32, jnp.bfloat16


def in_vmem(array):
    return pltpu.with_memory_space_constraint(array, pltpu.VMEM)


def specs(*kinds):
    return [pl.BlockSpec(memory_space=kind) for kind in kinds]


def pack_kernel(far, near, share, subdim, residuals, codes, out):
    lines = subdim + 1
    labels = codes[...].astype(f32).T
    local = labels.shape[0]
    span = 128 // subdim
    for first in range(0, local, span):
        piece = residuals[:, first * subdim : (first + span) * subdim].astype(f32).T
        for i in range(span):
            m = first + i
            w, s = m // share, m % share
            j = ((w % far) * near + w // far) * share + s
            out[lines * j : lines * j + subdim, :] = piece[subdim * i : subdim * (i + 1), :]
            out[lines * j + subdim : lines * (j + 1), :] = labels[m : m + 1, :]


def pack(residuals, codes, far, near):
    rows, local = codes.shape
    subdim = residuals.shape[1] // local
    return pl.pallas_call(
        functools.partial(pack_kernel, far, near, local // (far * near), subdim),
        out_specs=pl.BlockSpec(memory_space=pltpu.VMEM),
        out_shape=pltpu.VMEM((local * (subdim + 1), rows), f32),
    )(residuals, codes)


def send_sums(out, grid, s, total, share, lines):
    grid[s, :, 0 : total.shape[1]] = total
    sums = grid[s].T[0:lines, :]
    for c in range(out.shape[0] // (share * lines)):
        at = (c * share + s) * lines
        out[at : at + lines, :] = sums


def refreshed(before, parts, s, lam, share, lines):
    sums = parts[s * lines : (s + 1) * lines, :]
    for c in range(1, parts.shape[0] // (share * lines)):
        at = (c * share + s) * lines
        sums = sums + parts[at : at + lines, :]
    return (sums[0 : lines - 1, :] + lam * before) / (sums[lines - 1 : lines, :] + lam)


def first_kernel(subdim, width, share, own, data, codebook, out, x, prior, grid, arrived):
    fetch = pltpu.make_async_copy(codebook.at[pl.ds(own[0], share)], prior, arrived)
    fetch.start()
    lines = subdim + 1
    sources = data.shape[0] // (lines * share)
    span = data.shape[1]
    code_span = 16
    grid[...] = jnp.zeros_like(grid)
    levels = lax.broadcasted_iota(jnp.int32, (width, span), 0).astype(f32)
    ones = jnp.ones((subdim, span), f32)
    for s in range(share):
        total = jnp.zeros((width, 2 * subdim), f32)
        for start in range(0, sources, code_span):
            onehots, pieces = [], []
            for r in range(start, start + code_span):
                top = (r * share + s) * lines
                piece = data[top : top + subdim, :]
                counted = jnp.concatenate([piece, ones], axis=0).astype(bf16)
                at = slice(span * r, span * (r + 1))
                x[s, 0 : 2 * subdim, at] = jnp.concatenate([piece, piece], axis=0).astype(bf16)
                x[s, 2 * subdim : 4 * subdim, at] = counted
                pieces.append(counted)
                onehots.append(jnp.where(levels == data[top + subdim : top + lines, :], 1.0, 0.0).astype(bf16))
            onehot, piece = jnp.concatenate(onehots, axis=1), jnp.concatenate(pieces, axis=1)
            total += lax.dot_general(onehot, piece, NT, preferred_element_type=f32)
        send_sums(out, grid, s, total, share, lines)
    fetch.wait()


def first(own, data, codebook, blocks, share):
    _, subdim, width = codebook.shape
    lines = subdim + 1
    vectors = data.shape[0] // (lines * share) * data.shape[1]
    return pl.pallas_call(
        functools.partial(first_kernel, subdim, width, share),
        in_specs=specs(pltpu.SMEM, pltpu.VMEM, pl.ANY),
        out_specs=specs(pltpu.VMEM, pltpu.VMEM, pltpu.VMEM),
        scratch_shapes=[pltpu.VMEM((share, 128, 128), f32), pltpu.SemaphoreType.DMA],
        out_shape=[
            pltpu.VMEM((blocks * share * lines, width), f32),
            pltpu.VMEM((share, 4 * subdim, vectors), bf16),
            pltpu.VMEM((share, subdim, width), f32),
        ],
    )(own, in_vmem(data), codebook)


def thirds(value):
    head = value.astype(bf16).astype(f32)
    middle = (value - head).astype(bf16).astype(f32)
    return [head, middle, (value - head - middle).astype(bf16).astype(f32)]


def second_kernel(lam, subdim, width, share, parts, x, prior, out, book1, grid):
    lines = subdim + 1
    step = 256
    log2e = 1.4426950408889634
    grid[...] = jnp.zeros_like(grid)
    lefts = []
    for s in range(share):
        book = refreshed(prior[s], parts, s, lam, share, lines)
        book1[s] = book
        center = (2.0 * log2e) * book.astype(bf16).astype(f32)
        norm = -log2e * jnp.sum(book * book, axis=0, keepdims=True)
        rest = jnp.zeros((subdim - 3, width), f32)
        grid[s, 0 : 4 * subdim, :] = jnp.concatenate([*thirds(center), *thirds(norm), rest], axis=0)
        lefts.append(grid[s].T[:, 0 : 4 * subdim].astype(bf16))
    for s in range(share):
        total = jnp.zeros((width, 2 * subdim), f32)
        for at in range(0, x.shape[2], step):
            piece = x[s, :, at : at + step]
            scores = jnp.dot(lefts[s], piece, preferred_element_type=f32)
            scores = jnp.exp2(scores - jnp.max(scores, axis=0, keepdims=True))
            weights = (scores * (1.0 / jnp.sum(scores, axis=0, keepdims=True))).astype(bf16)
            total += lax.dot_general(weights, piece[2 * subdim : 4 * subdim], NT, preferred_element_type=f32)
        send_sums(out, grid, s, total, share, lines)


def second(parts, x, prior, lam):
    share, subdim, width = prior.shape
    return pl.pallas_call(
        functools.partial(second_kernel, lam, subdim, width, share),
        in_specs=specs(pltpu.VMEM, pltpu.VMEM, pltpu.VMEM),
        out_specs=specs(pltpu.VMEM, pltpu.VMEM),
        scratch_shapes=[pltpu.VMEM((share, 128, 128), f32)],
        out_shape=[pltpu.VMEM(parts.shape, f32), pltpu.VMEM(prior.shape, f32)],
    )(in_vmem(parts), in_vmem(x), in_vmem(prior))


def last_kernel(lam, parts, book1, out):
    share, subdim, _ = book1.shape
    for s in range(share):
        refined = refreshed(book1[s], parts, s, lam, share, subdim + 1)
        for c in range(out.shape[0]):
            out[c, s] = refined


def last(parts, book1, lam, copies):
    return pl.pallas_call(
        functools.partial(last_kernel, lam),
        in_specs=specs(pltpu.VMEM, pltpu.VMEM),
        out_specs=pl.BlockSpec(memory_space=pltpu.VMEM),
        out_shape=pltpu.VMEM((copies, *book1.shape), f32),
    )(in_vmem(parts), in_vmem(book1))


def exchanged(array, axes, blocks):
    return lax.all_to_all(array.reshape(blocks, 1, -1), axes, 0, 0, tiled=True).reshape(array.shape)


def shards(residuals, codes, codebook):
    rows, local = codes.shape
    blocks, far, near = (lax.axis_size(axis) for axis in ROWS)
    share = local // (far * near)
    lam = rows * blocks * far * near / (8.0 * codebook.shape[2])
    own = (lax.axis_index(ROWS[2]) * far + lax.axis_index(ROWS[1])) * share
    own = own.astype(jnp.int32).reshape(1)
    packed, own = lax.optimization_barrier((pack(residuals, codes, far, near), own))
    data = exchanged(packed, ROWS[1:], far * near)
    sums1, x, prior = first(own, data, codebook, blocks, share)
    sums2, book1 = second(exchanged(sums1, ROWS[0], blocks), x, prior, lam)
    books = last(exchanged(sums2, ROWS[0], blocks), book1, lam, far)
    books = lax.all_to_all(books, ROWS[1], 0, 0, tiled=True)
    books = lax.all_to_all(jnp.broadcast_to(books, (near, *books.shape)), ROWS[2], 0, 0, tiled=True)
    return books.reshape(codebook.shape)


def solution(mesh):
    split = Mesh(
        mesh.devices.reshape(mesh.shape["groups"], 4, 8, 4, mesh.shape["sub"]),
        (*GROUPS_ROWS, "sub"),
    )
    placed = (P(GROUPS_ROWS, "sub"), P(GROUPS_ROWS, "sub"), P(("groups", "sub"), None, None))
    return jax.shard_map(
        shards,
        mesh=split,
        in_specs=placed,
        out_specs=P(("groups", "sub"), None, None),
        check_vma=False,
    )
```
